64 devices in a mesh: dp: 8 (over x, y, core), sp: 8 (over z).
Axes of the slice: x: 2, y: 2, z: 8, core: 2. Of those that a mesh axis runs over, the one named last changes fastest.
The devices are a block of a 4x4x8 slice.
Arguments:
- q: bfloat16 [256, 32, 64], P('dp'), parts along dimension 0
- k: bfloat16 [256, 8192, 8, 64], P('dp', 'sp'), parts along dimension 0
- v: bfloat16 [256, 8192, 8, 64], P('dp', 'sp'), parts along dimension 0
Outputs:
- q: bfloat16 [256, 32, 64], P('dp'), parts along dimension 0
There are 8 independent parts. The reference program is written for one: setup_inputs(seed, part) draws one part's arguments, and reference() takes and returns one part's arrays. A program takes and returns all parts, laid end to end along the dimension named above; each array names one.
All inputs are finite; a program needn't handle non-finite values.
Results may differ from the reference program's by a relative error of at most 0.012.
Values are sent between devices in bfloat16 or wider.
A program may use at most 768 MiB of HBM per device.

```python
import jax
import jax.numpy as jnp

BATCH = 32
CACHE = 8192
HEADS = 32
KV_HEADS = 8
HEAD = 64


def setup_inputs(seed: int = 0, part: int = 0) -> dict:
    kq, kk, kv = (jax.random.fold_in(k, part) for k in jax.random.split(jax.random.key(seed), 3))
    return {
        "q": (3 * jax.random.normal(kq, (BATCH, HEADS, HEAD), jnp.float32)).astype(jnp.bfloat16),
        "k": jax.random.normal(kk, (BATCH, CACHE, KV_HEADS, HEAD), jnp.float32).astype(jnp.bfloat16),
        "v": jax.random.normal(kv, (BATCH, CACHE, KV_HEADS, HEAD), jnp.float32).astype(jnp.bfloat16),
    }


def einsum(form, a, b):
    return jnp.einsum(form, a.astype(jnp.float32), b.astype(jnp.float32))


def reference(q, k, v):
    grouped = q.reshape(BATCH, KV_HEADS, -1, HEAD)
    scores = einsum("bgsd,bugd->bgsu", grouped, k) * HEAD**-0.5
    weights = jax.nn.softmax(scores, -1).astype(jnp.bfloat16)
    return einsum("bgsu,bugd->bgsd", weights, v).astype(jnp.bfloat16).reshape(BATCH, HEADS, HEAD)
```

```python
import functools
import math

import jax
import jax.numpy as jnp
from jax import lax
from jax.experimental import pallas as pl
from jax.experimental.pallas import tpu as pltpu
from jax.sharding import PartitionSpec as P

SLOTS = 6
STEP = 2


def kernel(
    devices, rounds, q_hbm, k_hbm, v_hbm, out_ref,
    q_ref, keys, values, scores, part, stat, parts, stats, done,
    q_sem, k_sem, v_sem, send_part, send_stat, recv_part, recv_stat, send_done, recv_done,
):
    sequences, heads, depth = q_hbm.shape
    shared = rounds * devices
    factor = depth**-0.5 * math.log2(math.e)
    me = lax.axis_index("sp")
    order = sorted(range(1, devices), key=lambda d: -min(d, devices - d))

    def device(i):
        return {"sp": i}

    def fetch(hbm, buffer, sem, s):
        slot = lax.rem(s, SLOTS)
        return pltpu.make_async_copy(hbm.at[s], buffer.at[slot], sem.at[slot])

    def fetch_k(s):
        return fetch(k_hbm, keys, k_sem, s)

    def fetch_v(s):
        return fetch(v_hbm, values, v_sem, s)

    fetch_q = pltpu.make_async_copy(q_hbm, q_ref, q_sem)
    fetch_q.start()
    for s in range(SLOTS):
        fetch_k(s).start()
        fetch_v(s).start()
    barrier = pltpu.get_barrier_semaphore()
    for d in order:
        pl.semaphore_signal(barrier, inc=1, device_id=device(lax.rem(me + d, devices)), device_id_type=pl.DeviceIdType.MESH)

    half = heads // 2
    own = lax.broadcasted_iota(jnp.int32, (half, 4 * depth), 0) // 4 == lax.broadcasted_iota(jnp.int32, (half, 4 * depth), 1) // depth
    lane = lax.broadcasted_iota(jnp.int32, (8, 128), 1)
    row = lax.broadcasted_iota(jnp.int32, (8, 128), 0)
    left, upper = lane < 64, row < 4
    lane32 = lax.broadcasted_iota(jnp.int32, (32, 128), 1)
    row32 = lax.broadcasted_iota(jnp.int32, (32, 128), 0)
    place = lax.rem(row32 // 4, 2) * 16 + row32 // 8 * 4 + lax.rem(row32, 4)
    lane16 = lax.broadcasted_iota(jnp.int32, (16, 128), 1)
    row16 = lax.broadcasted_iota(jnp.int32, (16, 128), 0)

    def score(s, slot):
        q = q_ref[s]
        q = jnp.concatenate([q, q], 1)
        q = jnp.concatenate([q, q], 1)
        for g in range(2):
            rows = pl.ds(half * g, half)
            mine = jnp.where(own, q[half * g : half * (g + 1)].astype(jnp.float32), 0.0).astype(jnp.bfloat16)
            block = keys[lax.rem(s, SLOTS), pl.ds(4 * depth * g, 4 * depth), :]
            scores[slot, rows, :] = jnp.dot(mine, block, preferred_element_type=jnp.float32)

    def attend(s, slot):
        seen, highs, totals = [], [], []
        for g in range(2):
            x = scores[slot, pl.ds(half * g, half), :]
            high = jnp.max(x, -1, keepdims=True)
            weights = jnp.exp2((x - high) * factor)
            highs.append(high)
            totals.append(jnp.sum(weights, -1, keepdims=True))
            block = values[lax.rem(s, SLOTS), pl.ds(4 * depth * g, 4 * depth), :]
            o = lax.dot_general(weights.astype(jnp.bfloat16), block, (((1,), (1,)), ((), ())), preferred_element_type=jnp.float32)
            a, b = o[:8, :128], o[8:, 128:]
            a = jnp.where(left, a, pltpu.roll(a, 4, 0))
            b = jnp.where(left, pltpu.roll(b, 4, 0), b)
            seen.append(jnp.where(upper, a, b))
        part[s] = jnp.concatenate(seen, 0).astype(jnp.bfloat16)
        both = jnp.where(lane32 == place, jnp.concatenate(highs, 0), 0.0) + jnp.where(lane32 == place + 32, jnp.concatenate(totals, 0), 0.0)
        stat[s] = jnp.sum(both, 0, keepdims=True)

    def send(s, slot, to):
        pltpu.make_async_remote_copy(part.at[s], parts.at[slot, me], send_part.at[slot], recv_part.at[slot], device(to), pl.DeviceIdType.MESH).start()
        pltpu.make_async_remote_copy(stat.at[s], stats.at[slot, me], send_stat.at[slot], recv_stat.at[slot], device(to), pl.DeviceIdType.MESH).start()

    def leave(s):
        @pl.when(s < shared)
        def _():
            owner = lax.rem(s, devices)

            @pl.when(owner != me)
            def _():
                send(s, s // devices, owner)

        @pl.when(s >= shared)
        def _():
            for d in order:
                send(s, rounds + s - shared, lax.rem(me + d, devices))

    def others(ref, slot, sends, recvs):
        some = ref.at[slot, pl.ds(0, devices - 1)]
        return pltpu.make_async_remote_copy(some, some, sends.at[slot], recvs.at[slot], device(lax.rem(me + 1, devices)), pl.DeviceIdType.MESH)

    def together(slot, s):
        parts[slot, me] = part[s]
        stats[slot, me] = stat[s]
        others(parts, slot, send_part, recv_part).wait_recv()
        others(stats, slot, send_stat, recv_stat).wait_recv()
        st = stats[slot].reshape(devices, 128)
        scale = jnp.exp2((st - jnp.max(st, 0, keepdims=True)) * factor)
        total = jnp.sum(scale * pltpu.roll(st, 96, 1), 0, keepdims=True)
        scale = scale / total
        out = jnp.zeros((16, 128), jnp.float32)
        for j in range(devices):
            one = scale[j : j + 1]
            even = jnp.sum(jnp.where(lane16 == row16, one, 0.0), 1, keepdims=True)
            odd = jnp.sum(jnp.where(lane16 == row16 + 16, one, 0.0), 1, keepdims=True)
            out = out + parts[slot, j].astype(jnp.float32) * jnp.where(lane16 < 64, even, odd)
        return out

    def write(s, x):
        rows = []
        for j in range(2):
            v = x[8 * j : 8 * (j + 1)]
            w = pltpu.roll(v, 64, 1)
            rows += [jnp.where(upper, v, pltpu.roll(w, 4, 0)), jnp.where(upper, pltpu.roll(v, 4, 0), w)]
        out_ref[s] = jnp.concatenate(rows, 0).astype(jnp.bfloat16)

    def share(r):
        s = r * devices + me
        done[r, me] = together(r, s).astype(jnp.bfloat16)
        for d in order:
            to = lax.rem(me + d, devices)
            pltpu.make_async_remote_copy(done.at[r, me], done.at[r, me], send_done.at[r], recv_done.at[r], device(to), pl.DeviceIdType.MESH).start()

    fetch_q.wait()
    for u in range(STEP):
        fetch_k(u).wait()
        score(u, u)
    for u in range(STEP):
        fetch_k(u + SLOTS).start()

    steps = sequences // STEP
    turn = devices // STEP

    def body(i, _):
        s = i * STEP
        now = lax.rem(i, 2) * STEP

        @pl.when(i == 1)
        def _():
            pl.semaphore_wait(barrier, devices - 1)

        @pl.when(i > 0)
        def _():
            for u in range(STEP):
                leave(s - STEP + u)

        for r in range(rounds):
            @pl.when(i == turn * r + 2 * turn - 1)
            def _():
                share(r)

        @pl.when(i < steps - 1)
        def _():
            for u in range(STEP):
                fetch_k(s + STEP + u).wait()

        for u in range(STEP):
            fetch_v(s + u).wait()
        for u in range(STEP):
            score(jnp.minimum(s + STEP + u, sequences - 1), STEP - now + u)
        for u in range(STEP):
            attend(s + u, now + u)
        for u in range(STEP):
            t = s + STEP + SLOTS + u

            @pl.when(t < sequences)
            def _():
                fetch_k(t).start()

            @pl.when(t - STEP < sequences)
            def _():
                fetch_v(t - STEP).start()

        return 0

    lax.fori_loop(0, steps, body, 0)
    for u in range(STEP):
        leave(sequences - STEP + u)

    for r in range(rounds):
        others(done, r, send_done, recv_done).wait_recv()

        def emit(j, _):
            write(r * devices + j, done[r, j].astype(jnp.float32))
            return 0

        lax.fori_loop(0, devices, emit, 0)

    def finish(j, _):
        write(shared + j, together(rounds + j, shared + j))
        return 0

    lax.fori_loop(0, sequences - shared, finish, 0)

    for r in range(rounds):
        others(done, r, send_done, recv_done).wait_send()

    def drain(slot, _):
        others(parts, slot, send_part, recv_part).wait_send()
        others(stats, slot, send_stat, recv_stat).wait_send()
        return 0

    lax.fori_loop(0, rounds + sequences - shared, drain, 0)


def solution(mesh):
    devices = mesh.shape["sp"]

    def step(q, k, v):
        n, heads, depth = q.shape
        tokens, groups = k.shape[1:3]
        rounds = n // devices - 1
        slots = rounds + devices
        k, v = (x.transpose(0, 2, 3, 1).reshape(n, groups * depth, tokens) for x in (k, v))
        out = pl.pallas_call(
            functools.partial(kernel, devices, rounds),
            out_shape=jax.ShapeDtypeStruct((n, heads, 128), jnp.bfloat16),
            in_specs=[pl.BlockSpec(memory_space=pl.ANY)] * 3,
            out_specs=pl.BlockSpec(memory_space=pltpu.VMEM),
            scratch_shapes=[
                pltpu.VMEM((n, heads, depth), jnp.bfloat16),
                pltpu.VMEM((SLOTS, groups * depth, tokens), jnp.bfloat16),
                pltpu.VMEM((SLOTS, groups * depth, tokens), jnp.bfloat16),
                pltpu.VMEM((2 * STEP, heads, tokens), jnp.float32),
                pltpu.VMEM((n, 16, 128), jnp.bfloat16),
                pltpu.VMEM((n, 1, 128), jnp.float32),
                pltpu.VMEM((slots, devices, 16, 128), jnp.bfloat16),
                pltpu.VMEM((slots, devices, 1, 128), jnp.float32),
                pltpu.VMEM((rounds, devices, 16, 128), jnp.bfloat16),
                pltpu.SemaphoreType.DMA,
                pltpu.SemaphoreType.DMA((SLOTS,)),
                pltpu.SemaphoreType.DMA((SLOTS,)),
                pltpu.SemaphoreType.DMA((slots,)),
                pltpu.SemaphoreType.DMA((slots,)),
                pltpu.SemaphoreType.DMA((slots,)),
                pltpu.SemaphoreType.DMA((slots,)),
                pltpu.SemaphoreType.DMA((rounds,)),
                pltpu.SemaphoreType.DMA((rounds,)),
            ],
            compiler_params=pltpu.CompilerParams(collective_id=0, has_side_effects=True, vmem_limit_bytes=60 * 2**20),
        )(q, k, v)
        return out[:, :, :depth]

    return jax.shard_map(
        step,
        mesh=mesh,
        in_specs=(P("dp", None, None), P("dp", "sp", None, None), P("dp", "sp", None, None)),
        out_specs=P("dp", None, None),
        check_vma=False,
    )
```

```python
import functools
import math

import jax
import jax.numpy as jnp
from jax import lax
from jax.experimental import pallas as pl
from jax.experimental.pallas import tpu as pltpu
from jax.sharding import PartitionSpec as P

SLOTS = 6
STEP = 2
DIRECT = 2
GREET = 3


def kernel(
    devices, q_hbm, k_hbm, v_hbm, out_ref,
    q_ref, keys, values, scores, part, stat, owner_parts, owner_stats, parts, stats, done,
    q_sem, k_sem, v_sem, send_part, send_stat, owner_recv_part, owner_recv_stat, recv_part, recv_stat, send_done, recv_done,
):
    sequences, heads, depth = q_hbm.shape
    shared = sequences - DIRECT
    spread = 2 * devices
    front = devices // 2
    near = spread + front
    factor = depth**-0.5 * math.log2(math.e)
    me = lax.axis_index("sp")
    order = sorted(range(1, devices), key=lambda d: -min(d, devices - d))

    def device(i):
        return {"sp": i}

    def fetch(hbm, buffer, sem, s):
        slot = lax.rem(s, SLOTS)
        return pltpu.make_async_copy(hbm.at[s], buffer.at[slot], sem.at[slot])

    def in_pieces(hbm, buffer, sem, s):
        slot = lax.rem(s, SLOTS)
        size = buffer.shape[1] // 4
        for piece in range(4):
            rows = pl.ds(piece * size, size)
            pltpu.make_async_copy(hbm.at[s, rows], buffer.at[slot, rows], sem.at[slot]).start()

    def fetch_k(s):
        return fetch(k_hbm, keys, k_sem, s)

    def fetch_v(s):
        return fetch(v_hbm, values, v_sem, s)

    fetch_q = pltpu.make_async_copy(q_hbm, q_ref, q_sem)
    fetch_q.start()
    for u in range(STEP):
        fetch_k(u).start()
    for u in range(STEP):
        fetch_v(u).start()
    barrier = pltpu.get_barrier_semaphore()
    for d in order:
        pl.semaphore_signal(barrier, inc=1, device_id=device(lax.rem(me + d, devices)), device_id_type=pl.DeviceIdType.MESH)

    half = heads // 2
    own = lax.broadcasted_iota(jnp.int32, (half, 4 * depth), 0) // 4 == lax.broadcasted_iota(jnp.int32, (half, 4 * depth), 1) // depth
    lane = lax.broadcasted_iota(jnp.int32, (8, 128), 1)
    row = lax.broadcasted_iota(jnp.int32, (8, 128), 0)
    left, upper = lane < 64, row < 4
    lane32 = lax.broadcasted_iota(jnp.int32, (32, 128), 1)
    row32 = lax.broadcasted_iota(jnp.int32, (32, 128), 0)
    place = lax.rem(row32 // 4, 2) * 16 + row32 // 8 * 4 + lax.rem(row32, 4)
    lane16 = lax.broadcasted_iota(jnp.int32, (16, 128), 1)
    row16 = lax.broadcasted_iota(jnp.int32, (16, 128), 0)

    def score(s, slot):
        q = q_ref[s]
        q = jnp.concatenate([q, q], 1)
        q = jnp.concatenate([q, q], 1)
        for g in range(2):
            rows = pl.ds(half * g, half)
            mine = jnp.where(own, q[half * g : half * (g + 1)].astype(jnp.float32), 0.0).astype(jnp.bfloat16)
            block = keys[lax.rem(s, SLOTS), pl.ds(4 * depth * g, 4 * depth), :]
            scores[slot, rows, :] = jnp.dot(mine, block, preferred_element_type=jnp.float32)

    def attend(s, slot):
        seen, highs, totals = [], [], []
        for g in range(2):
            x = scores[slot, pl.ds(half * g, half), :]
            high = jnp.max(x, -1, keepdims=True)
            weights = jnp.exp2((x - high) * factor)
            highs.append(high)
            totals.append(jnp.sum(weights, -1, keepdims=True))
            block = values[lax.rem(s, SLOTS), pl.ds(4 * depth * g, 4 * depth), :]
            o = lax.dot_general(weights.astype(jnp.bfloat16), block, (((1,), (1,)), ((), ())), preferred_element_type=jnp.float32)
            a, b = o[:8, :128], o[8:, 128:]
            a = jnp.where(left, a, pltpu.roll(a, 4, 0))
            b = jnp.where(left, pltpu.roll(b, 4, 0), b)
            seen.append(jnp.where(upper, a, b))
        part[s] = jnp.concatenate(seen, 0).astype(jnp.bfloat16)
        both = jnp.where(lane32 == place, jnp.concatenate(highs, 0), 0.0) + jnp.where(lane32 == place + 32, jnp.concatenate(totals, 0), 0.0)
        stat[s] = jnp.sum(both, 0, keepdims=True)

    def owner_of(s):
        late = jnp.maximum(0, front - 1 - (s - near) // STEP)
        return jnp.where(s < spread, lax.rem(s, devices), jnp.where(s < near, s - spread + front, late))

    def first_of(d):
        return near + (front - 1 - d) * STEP

    def slot_of(s):
        return jnp.where(s < spread, s // devices, jnp.where(s < near, 2, 2 + s - first_of(owner_of(s))))

    def remote(src, dst, send, recv, to):
        return pltpu.make_async_remote_copy(src, dst, send, recv, device(to), pl.DeviceIdType.MESH)

    def leave(i):
        for u in range(STEP):
            s = i * STEP + u
            owner = jnp.where(i < spread // STEP, lax.rem(i * STEP, devices) + u, jnp.where(i < near // STEP, s - spread + front, jnp.maximum(0, front - 1 + near // STEP - i)))
            more = jnp.maximum(0, i - (near // STEP + front - 1)) * STEP + u
            slot = jnp.where(i < spread // STEP, i * STEP // devices, jnp.where(i < near // STEP, 2, 2 + more))

            @pl.when(owner != me)
            def _():
                remote(part.at[s], owner_parts.at[me, slot], send_part.at[s], owner_recv_part.at[slot], owner).start()
                remote(stat.at[s], owner_stats.at[me, slot], send_stat.at[s], owner_recv_stat.at[slot], owner).start()

    def leave_all(s):
        here, there = pl.ds(s, STEP), pl.ds(s - shared, STEP)
        t = (s - shared) // STEP
        for d in order:
            to = lax.rem(me + d, devices)
            remote(part.at[here], parts.at[me, there], send_part.at[s], recv_part.at[t], to).start()
            remote(stat.at[here], stats.at[me, there], send_stat.at[s], recv_stat.at[t], to).start()

    neighbour = lax.rem(me + 1, devices)

    def arrived(part_block, stat_block, part_sem, stat_sem):
        remote(part_block, part_block, send_part.at[0], part_sem, neighbour).wait_recv()
        remote(stat_block, stat_block, send_stat.at[0], stat_sem, neighbour).wait_recv()

    most = pl.ds(0, devices - 1)

    def together(parts, stats, slot, s):
        parts[me, slot] = part[s]
        stats[me, slot] = stat[s]
        st = stats[:, slot].reshape(devices, 128)
        scale = jnp.exp2((st - jnp.max(st, 0, keepdims=True)) * factor)
        total = jnp.sum(scale * pltpu.roll(st, 96, 1), 0, keepdims=True)
        scale = scale / total
        out = jnp.zeros((16, 128), jnp.float32)
        for j in range(devices):
            one = scale[j : j + 1]
            even = jnp.sum(jnp.where(lane16 == row16, one, 0.0), 1, keepdims=True)
            odd = jnp.sum(jnp.where(lane16 == row16 + 16, one, 0.0), 1, keepdims=True)
            out = out + parts[j, slot].astype(jnp.float32) * jnp.where(lane16 < 64, even, odd)
        return out

    def write(s, x):
        rows = []
        for j in range(2):
            v = x[8 * j : 8 * (j + 1)]
            w = pltpu.roll(v, 64, 1)
            rows += [jnp.where(upper, v, pltpu.roll(w, 4, 0)), jnp.where(upper, pltpu.roll(v, 4, 0), w)]
        out_ref[s] = jnp.concatenate(rows, 0).astype(jnp.bfloat16)

    def share(s):
        r = slot_of(s)
        arrived(owner_parts.at[most, 0], owner_stats.at[most, 0], owner_recv_part.at[r], owner_recv_stat.at[r])
        done[s] = together(owner_parts, owner_stats, r, s).astype(jnp.bfloat16)
        for d in order:
            remote(done.at[s], done.at[s], send_done.at[r], recv_done.at[jnp.where(s < spread, s // devices, s)], lax.rem(me + d, devices)).start()

    fetch_q.wait()
    for u in range(STEP):
        fetch_k(STEP + u).start()
    for u in range(STEP):
        fetch_k(u).wait()
        score(u, u)
        for t in range(STEP):
            (fetch_k(2 * STEP + t) if u else fetch_v(STEP + t)).start()
    for u in range(STEP):
        fetch_v(u).wait()
    for u in range(STEP):
        attend(u, u)
    for u in range(STEP):
        fetch_v(2 * STEP + u).start()
        fetch_k(3 * STEP + u).start()
    for u in range(STEP):
        fetch_k(STEP + u).wait()
    for u in range(STEP):
        score(STEP + u, STEP + u)
    for u in range(STEP):
        fetch_v(3 * STEP + u).start()
        fetch_k(4 * STEP + u).start()

    steps = sequences // STEP

    def body(i, _):
        s = i * STEP
        now = lax.rem(i, 2) * STEP

        for u in range(STEP):
            fetch_k(s + STEP + u).wait()
            fetch_v(s + u).wait()
        for u in range(STEP):
            score(s + STEP + u, STEP - now + u)
        for u in range(STEP):
            attend(s + u, now + u)
        @pl.when(s + STEP + SLOTS < sequences)
        def _():
            for u in range(STEP):
                fetch_k(s + STEP + SLOTS + u).start()
                fetch_v(s + SLOTS + u).start()

        @pl.when(s + STEP + SLOTS == sequences)
        def _():
            in_pieces(v_hbm, values, v_sem, s + SLOTS)
            for u in range(1, STEP):
                fetch_v(s + SLOTS + u).start()

        @pl.when(i == GREET)
        def _():
            pl.semaphore_wait(barrier, devices - 1)

            def first(t, _):
                leave(t)
                return 0

            lax.fori_loop(0, GREET, first, 0)

        @pl.when(i >= GREET)
        def _():
            leave(i)

        early = devices - 1 - me

        @pl.when(i == 6 + early)
        def _():
            share(me)

        @pl.when((i == 10 + early) & (me >= front))
        def _():
            share(devices + me)

        @pl.when((i == 12 + early // 2) & (me >= front))
        def _():
            share(spread - front + me)

        return 0

    lax.fori_loop(1, steps - 1, body, 0)
    last = sequences - STEP
    for u in range(STEP):
        fetch_v(last + u).wait()
        attend(last + u, last % (2 * STEP) + u)
    leave_all(last)

    def emit_round(r):
        block = done.at[most]
        remote(block, block, send_done.at[0], recv_done.at[r], neighbour).wait_recv()
        for d in range(devices):
            write(r * devices + d, done[r * devices + d].astype(jnp.float32))

    def sent(s, _):
        @pl.when(owner_of(s) != me)
        def _():
            remote(part.at[s], part.at[s], send_part.at[s], recv_part.at[0], neighbour).wait_send()
            remote(stat.at[s], stat.at[s], send_stat.at[s], recv_stat.at[0], neighbour).wait_send()

        return 0

    @pl.when(me < front)
    def _():
        share(devices + me)

    emit_round(0)
    lax.fori_loop(0, shared, sent, 0)

    @pl.when(me < front)
    def _():
        def each(s, _):
            share(s)
            return 0

        lax.fori_loop(first_of(me), jnp.where(me == 0, shared, first_of(me) + STEP), each, 0)

    emit_round(1)

    def come(s, _):
        @pl.when(owner_of(s) != me)
        def _():
            remote(done.at[s], done.at[s], send_done.at[0], recv_done.at[s], neighbour).wait_recv()

        return 0

    lax.fori_loop(spread, shared, come, 0)
    for s in range(spread, shared):
        write(s, done[s].astype(jnp.float32))

    def finish(t, _):
        arrived(parts.at[most, pl.ds(0, STEP)], stats.at[most, pl.ds(0, STEP)], recv_part.at[t], recv_stat.at[t])
        for u in range(STEP):
            write(shared + t * STEP + u, together(parts, stats, t * STEP + u, shared + t * STEP + u))
        return 0

    def sent_all(t, _):
        s = shared + t * STEP
        block = parts.at[most, pl.ds(0, STEP)]
        remote(block, block, send_part.at[s], recv_part.at[0], neighbour).wait_send()
        block = stats.at[most, pl.ds(0, STEP)]
        remote(block, block, send_stat.at[s], recv_stat.at[0], neighbour).wait_send()
        return 0

    lax.fori_loop(0, DIRECT // STEP, sent_all, 0)

    def shared_all(r, _):
        block = done.at[most]
        remote(block, block, send_done.at[r], recv_done.at[0], neighbour).wait_send()
        return 0

    lax.fori_loop(0, jnp.where(me >= front, 3, jnp.where(me == 0, 2 + shared - first_of(0), 2 + STEP)), shared_all, 0)
    finish(DIRECT // STEP - 1, 0)


def solution(mesh):
    devices = mesh.shape["sp"]

    def step(q, k, v):
        n, heads, depth = q.shape
        tokens, groups = k.shape[1:3]
        shared = n - DIRECT
        rounds = 2 + n - DIRECT - (5 * devices // 2 + (devices // 2 - 1) * STEP)
        k, v = (x.transpose(0, 2, 3, 1).reshape(n, groups * depth, tokens) for x in (k, v))
        out = pl.pallas_call(
            functools.partial(kernel, devices),
            out_shape=pltpu.VMEM((n, heads, 128), jnp.bfloat16),
            in_specs=[pl.BlockSpec(memory_space=pl.ANY)] * 3,
            out_specs=pl.BlockSpec(memory_space=pltpu.VMEM),
            scratch_shapes=[
                pltpu.VMEM((n, heads, depth), jnp.bfloat16),
                pltpu.VMEM((SLOTS, groups * depth, tokens), jnp.bfloat16),
                pltpu.VMEM((SLOTS, groups * depth, tokens), jnp.bfloat16),
                pltpu.VMEM((2 * STEP, heads, tokens), jnp.float32),
                pltpu.VMEM((n, 16, 128), jnp.bfloat16),
                pltpu.VMEM((n, 1, 128), jnp.float32),
                pltpu.VMEM((devices, rounds, 16, 128), jnp.bfloat16),
                pltpu.VMEM((devices, rounds, 1, 128), jnp.float32),
                pltpu.VMEM((devices, DIRECT, 16, 128), jnp.bfloat16),
                pltpu.VMEM((devices, DIRECT, 1, 128), jnp.float32),
                pltpu.VMEM((shared, 16, 128), jnp.bfloat16),
                pltpu.SemaphoreType.DMA,
                pltpu.SemaphoreType.DMA((SLOTS,)),
                pltpu.SemaphoreType.DMA((SLOTS,)),
                pltpu.SemaphoreType.DMA((n,)),
                pltpu.SemaphoreType.DMA((n,)),
                pltpu.SemaphoreType.DMA((rounds,)),
                pltpu.SemaphoreType.DMA((rounds,)),
                pltpu.SemaphoreType.DMA((DIRECT // STEP,)),
                pltpu.SemaphoreType.DMA((DIRECT // STEP,)),
                pltpu.SemaphoreType.DMA((rounds,)),
                pltpu.SemaphoreType.DMA((shared,)),
            ],
            compiler_params=pltpu.CompilerParams(collective_id=0, has_side_effects=True, vmem_limit_bytes=60 * 2**20),
        )(q, k, v)
        return out[:, :, :depth]

    return jax.shard_map(
        step,
        mesh=mesh,
        in_specs=(P("dp", None, None), P("dp", "sp", None, None), P("dp", "sp", None, None)),
        out_specs=P("dp", None, None),
        check_vma=False,
    )
```

```python
import functools
import math

import jax
import jax.numpy as jnp
from jax import lax
from jax.experimental import pallas as pl
from jax.experimental.pallas import tpu as pltpu
from jax.sharding import PartitionSpec as P

SLOTS = 6
STEP = 2
DIRECT = 2
GREET = 3


def kernel(
    devices, q_hbm, k_hbm, v_hbm, out_ref,
    q_ref, keys, values, scores, part, stat, owner_parts, owner_stats, parts, stats, done,
    q_sem, k_sem, v_sem, send_part, send_stat, owner_recv_part, owner_recv_stat, recv_part, recv_stat, send_done, recv_done,
):
    sequences, heads, depth = q_hbm.shape
    shared = sequences - DIRECT
    front = devices // 2
    spread = shared - (front + 1) * STEP
    turns = spread // front
    factor = depth**-0.5 * math.log2(math.e)
    me = lax.axis_index("sp")
    order = sorted(range(1, devices), key=lambda d: -min(d, devices - d))

    def device(i):
        return {"sp": i}

    def fetch(hbm, buffer, sem, s):
        slot = lax.rem(s, SLOTS)
        return pltpu.make_async_copy(hbm.at[s], buffer.at[slot], sem.at[slot])

    def in_pieces(hbm, buffer, sem, s):
        slot = lax.rem(s, SLOTS)
        size = buffer.shape[1] // 4
        for piece in range(4):
            rows = pl.ds(piece * size, size)
            pltpu.make_async_copy(hbm.at[s, rows], buffer.at[slot, rows], sem.at[slot]).start()

    def fetch_k(s):
        return fetch(k_hbm, keys, k_sem, s)

    def fetch_v(s):
        return fetch(v_hbm, values, v_sem, s)

    fetch_q = pltpu.make_async_copy(q_hbm, q_ref, q_sem)
    fetch_q.start()
    for u in range(STEP):
        fetch_k(u).start()
    for u in range(STEP):
        fetch_v(u).start()
    barrier = pltpu.get_barrier_semaphore()
    for d in order:
        pl.semaphore_signal(barrier, inc=1, device_id=device(lax.rem(me + d, devices)), device_id_type=pl.DeviceIdType.MESH)

    half = heads // 2
    own = lax.broadcasted_iota(jnp.int32, (half, 4 * depth), 0) // 4 == lax.broadcasted_iota(jnp.int32, (half, 4 * depth), 1) // depth
    lane = lax.broadcasted_iota(jnp.int32, (8, 128), 1)
    row = lax.broadcasted_iota(jnp.int32, (8, 128), 0)
    left, upper = lane < 64, row < 4
    lane32 = lax.broadcasted_iota(jnp.int32, (32, 128), 1)
    row32 = lax.broadcasted_iota(jnp.int32, (32, 128), 0)
    place = lax.rem(row32 // 4, 2) * 16 + row32 // 8 * 4 + lax.rem(row32, 4)
    lane16 = lax.broadcasted_iota(jnp.int32, (16, 128), 1)
    row16 = lax.broadcasted_iota(jnp.int32, (16, 128), 0)

    def score(s, slot):
        q = q_ref[s]
        q = jnp.concatenate([q, q], 1)
        q = jnp.concatenate([q, q], 1)
        for g in range(2):
            rows = pl.ds(half * g, half)
            mine = jnp.where(own, q[half * g : half * (g + 1)].astype(jnp.float32), 0.0).astype(jnp.bfloat16)
            block = keys[lax.rem(s, SLOTS), pl.ds(4 * depth * g, 4 * depth), :]
            scores[slot, rows, :] = jnp.dot(mine, block, preferred_element_type=jnp.float32)

    def attend(s, slot):
        seen, highs, totals = [], [], []
        for g in range(2):
            x = scores[slot, pl.ds(half * g, half), :]
            high = jnp.max(x, -1, keepdims=True)
            weights = jnp.exp2((x - high) * factor)
            highs.append(high)
            totals.append(jnp.sum(weights, -1, keepdims=True))
            block = values[lax.rem(s, SLOTS), pl.ds(4 * depth * g, 4 * depth), :]
            o = lax.dot_general(weights.astype(jnp.bfloat16), block, (((1,), (1,)), ((), ())), preferred_element_type=jnp.float32)
            a, b = o[:8, :128], o[8:, 128:]
            a = jnp.where(left, a, pltpu.roll(a, 4, 0))
            b = jnp.where(left, pltpu.roll(b, 4, 0), b)
            seen.append(jnp.where(upper, a, b))
        part[s] = jnp.concatenate(seen, 0).astype(jnp.bfloat16)
        both = jnp.where(lane32 == place, jnp.concatenate(highs, 0), 0.0) + jnp.where(lane32 == place + 32, jnp.concatenate(totals, 0), 0.0)
        stat[s] = jnp.sum(both, 0, keepdims=True)

    def first_of(d):
        return spread + (front - 1 - d) * STEP

    def remote(src, dst, send, recv, to):
        return pltpu.make_async_remote_copy(src, dst, send, recv, device(to), pl.DeviceIdType.MESH)

    def leave(i):
        j = i - spread // STEP
        for u in range(STEP):
            s = i * STEP + u
            owner = jnp.where(j < 0, lax.rem(s, front), jnp.maximum(0, front - 1 - j))
            slot = jnp.where(j < 0, s // front, turns + u + jnp.maximum(0, j - front + 1) * STEP)

            @pl.when(owner != me)
            def _():
                remote(part.at[s], owner_parts.at[me, slot], send_part.at[0], owner_recv_part.at[slot], owner).start()
                remote(stat.at[s], owner_stats.at[me, slot], send_stat.at[0], owner_recv_stat.at[slot], owner).start()

    def leave_all(s):
        here, there = pl.ds(s, STEP), pl.ds(s - shared, STEP)
        for d in order:
            to = lax.rem(me + d, devices)
            remote(part.at[here], parts.at[me, there], send_part.at[1], recv_part, to).start()
            remote(stat.at[here], stats.at[me, there], send_stat.at[1], recv_stat, to).start()

    neighbour = lax.rem(me + 1, devices)

    def arrived(part_block, stat_block, part_sem, stat_sem):
        remote(part_block, part_block, send_part.at[0], part_sem, neighbour).wait_recv()
        remote(stat_block, stat_block, send_stat.at[0], stat_sem, neighbour).wait_recv()

    most = pl.ds(0, devices - 1)

    def together(parts, stats, slot, s):
        parts[me, slot] = part[s]
        stats[me, slot] = stat[s]
        st = stats[:, slot].reshape(devices, 128)
        scale = jnp.exp2((st - jnp.max(st, 0, keepdims=True)) * factor)
        total = jnp.sum(scale * pltpu.roll(st, 96, 1), 0, keepdims=True)
        scale = scale / total
        out = jnp.zeros((16, 128), jnp.float32)
        for j in range(devices):
            one = scale[j : j + 1]
            even = jnp.sum(jnp.where(lane16 == row16, one, 0.0), 1, keepdims=True)
            odd = jnp.sum(jnp.where(lane16 == row16 + 16, one, 0.0), 1, keepdims=True)
            out = out + parts[j, slot].astype(jnp.float32) * jnp.where(lane16 < 64, even, odd)
        return out

    def write(s, x):
        rows = []
        for j in range(2):
            v = x[8 * j : 8 * (j + 1)]
            w = pltpu.roll(v, 64, 1)
            rows += [jnp.where(upper, v, pltpu.roll(w, 4, 0)), jnp.where(upper, pltpu.roll(v, 4, 0), w)]
        out_ref[s] = jnp.concatenate(rows, 0).astype(jnp.bfloat16)

    def share(s, slot, group):
        arrived(owner_parts.at[most, 0], owner_stats.at[most, 0], owner_recv_part.at[slot], owner_recv_stat.at[slot])
        done[s] = together(owner_parts, owner_stats, slot, s).astype(jnp.bfloat16)
        for d in order:
            remote(done.at[s], done.at[s], send_done, recv_done.at[group], lax.rem(me + d, devices)).start()

    fetch_q.wait()
    for u in range(STEP):
        fetch_k(STEP + u).start()
    for u in range(STEP):
        fetch_k(u).wait()
        score(u, u)
        for t in range(STEP):
            (fetch_k(2 * STEP + t) if u else fetch_v(STEP + t)).start()
    for u in range(STEP):
        fetch_v(u).wait()
    for u in range(STEP):
        attend(u, u)
    for u in range(STEP):
        fetch_v(2 * STEP + u).start()
        fetch_k(3 * STEP + u).start()
    for u in range(STEP):
        fetch_k(STEP + u).wait()
    for u in range(STEP):
        score(STEP + u, STEP + u)
    for u in range(STEP):
        fetch_v(3 * STEP + u).start()
        fetch_k(4 * STEP + u).start()

    steps = sequences // STEP

    def body(i, _):
        s = i * STEP
        now = lax.rem(i, 2) * STEP

        for u in range(STEP):
            fetch_k(s + STEP + u).wait()
            fetch_v(s + u).wait()
        for u in range(STEP):
            score(s + STEP + u, STEP - now + u)
        for u in range(STEP):
            attend(s + u, now + u)
        @pl.when(s + STEP + SLOTS < sequences)
        def _():
            for u in range(STEP):
                fetch_k(s + STEP + SLOTS + u).start()
                fetch_v(s + SLOTS + u).start()

        @pl.when(s + STEP + SLOTS == sequences)
        def _():
            in_pieces(v_hbm, values, v_sem, s + SLOTS)
            for u in range(1, STEP):
                fetch_v(s + SLOTS + u).start()

        @pl.when(i == GREET)
        def _():
            pl.semaphore_wait(barrier, devices - 1)

            def first(t, _):
                leave(t)
                return 0

            lax.fori_loop(0, GREET, first, 0)

        @pl.when(i >= GREET)
        def _():
            leave(i)

        return 0

    lax.fori_loop(1, steps - 1, body, 0)
    last = sequences - STEP
    for u in range(STEP):
        fetch_v(last + u).wait()
        attend(last + u, last % (2 * STEP) + u)
    leave_all(last)

    def await_done(group, count):
        block = done.at[pl.ds(0, count)]
        remote(block, block, send_done, recv_done.at[group], neighbour).wait_recv()

    def emit(first, end):
        for s in range(first, end):
            write(s, done[s].astype(jnp.float32))

    is_owner, is_first, is_middle = me < front, me == 0, (me > 0) & (me < front)

    @pl.when(is_owner)
    def _():
        def each(t, _):
            share(t * front + me, t, 0)
            return 0

        lax.fori_loop(0, turns, each, 0)
        for u in range(STEP):
            share(first_of(me) + u, turns + u, 1)

    def sent(count, own):
        remote(part.at[pl.ds(0, count)], part.at[pl.ds(0, count)], send_part.at[0], recv_part, neighbour).wait_send()
        remote(stat.at[pl.ds(0, count)], stat.at[pl.ds(0, count)], send_stat.at[0], recv_stat, neighbour).wait_send()
        if own:
            block = owner_parts.at[most, pl.ds(0, own)]
            remote(block, block, send_done, recv_part, neighbour).wait_send()

    @pl.when(is_first)
    def _():
        for u in range(STEP, 2 * STEP):
            share(first_of(0) + u, turns + u, 1)
        await_done(0, spread - turns)
        await_done(1, (front - 1) * STEP)
        sent(shared - turns - 2 * STEP, turns + 2 * STEP)

    @pl.when(is_middle)
    def _():
        await_done(0, spread - turns)
        sent(shared - turns - STEP, turns + STEP)
        await_done(1, front * STEP)

    @pl.when(jnp.logical_not(is_owner))
    def _():
        await_done(0, spread)
        sent(shared, 0)
        await_done(1, (front + 1) * STEP)

    emit(0, shared)
    some_parts, some_stats = parts.at[most, pl.ds(0, STEP)], stats.at[most, pl.ds(0, STEP)]
    remote(some_parts, some_parts, send_part.at[1], recv_part, neighbour).wait()
    remote(some_stats, some_stats, send_stat.at[1], recv_stat, neighbour).wait()
    for u in range(STEP):
        write(shared + u, together(parts, stats, u, shared + u))


def solution(mesh):
    devices = mesh.shape["sp"]

    def step(q, k, v):
        n, heads, depth = q.shape
        tokens, groups = k.shape[1:3]
        shared = n - DIRECT
        own = (shared - (devices // 2 + 1) * STEP) // (devices // 2) + 2 * STEP
        k, v = (x.transpose(0, 2, 3, 1).reshape(n, groups * depth, tokens) for x in (k, v))
        out = pl.pallas_call(
            functools.partial(kernel, devices),
            out_shape=pltpu.VMEM((n, heads, 128), jnp.bfloat16),
            in_specs=[pl.BlockSpec(memory_space=pl.ANY)] * 3,
            out_specs=pl.BlockSpec(memory_space=pltpu.VMEM),
            scratch_shapes=[
                pltpu.VMEM((n, heads, depth), jnp.bfloat16),
                pltpu.VMEM((SLOTS, groups * depth, tokens), jnp.bfloat16),
                pltpu.VMEM((SLOTS, groups * depth, tokens), jnp.bfloat16),
                pltpu.VMEM((2 * STEP, heads, tokens), jnp.float32),
                pltpu.VMEM((n, 16, 128), jnp.bfloat16),
                pltpu.VMEM((n, 1, 128), jnp.float32),
                pltpu.VMEM((devices, own, 16, 128), jnp.bfloat16),
                pltpu.VMEM((devices, own, 1, 128), jnp.float32),
                pltpu.VMEM((devices, DIRECT, 16, 128), jnp.bfloat16),
                pltpu.VMEM((devices, DIRECT, 1, 128), jnp.float32),
                pltpu.VMEM((shared, 16, 128), jnp.bfloat16),
                pltpu.SemaphoreType.DMA,
                pltpu.SemaphoreType.DMA((SLOTS,)),
                pltpu.SemaphoreType.DMA((SLOTS,)),
                pltpu.SemaphoreType.DMA((2,)),
                pltpu.SemaphoreType.DMA((2,)),
                pltpu.SemaphoreType.DMA((own,)),
                pltpu.SemaphoreType.DMA((own,)),
                pltpu.SemaphoreType.DMA,
                pltpu.SemaphoreType.DMA,
                pltpu.SemaphoreType.DMA,
                pltpu.SemaphoreType.DMA((2,)),
            ],
            compiler_params=pltpu.CompilerParams(collective_id=0, has_side_effects=True, vmem_limit_bytes=60 * 2**20),
        )(q, k, v)
        return out[:, :, :depth]

    return jax.shard_map(
        step,
        mesh=mesh,
        in_specs=(P("dp", None, None), P("dp", "sp", None, None), P("dp", "sp", None, None)),
        out_specs=P("dp", None, None),
        check_vma=False,
    )
```

```python
import functools
import math

import jax
import jax.numpy as jnp
from jax import lax
from jax.experimental import pallas as pl
from jax.experimental.pallas import tpu as pltpu
from jax.sharding import PartitionSpec as P

SLOTS = 6
STEP = 2
DIRECT = 2
GREET = 3


def kernel(
    devices, q_hbm, k_hbm, v_hbm, out_ref,
    q_ref, keys, values, scores, part, stat, owner_parts, owner_stats, parts, stats, done,
    q_sem, k_sem, v_sem, send_part, send_stat, owner_recv_part, owner_recv_stat, recv_part, recv_stat, send_done, recv_done,
):
    sequences, heads, depth = q_hbm.shape
    shared = sequences - DIRECT
    front = devices // 2
    spread = shared - (front + 1) * STEP
    turns = spread // front
    most_own = turns + 2 * STEP
    factor = depth**-0.5 * math.log2(math.e)
    me = lax.axis_index("sp")
    order = sorted(range(1, devices), key=lambda d: -min(d, devices - d))

    def device(i):
        return {"sp": i}

    def fetch(hbm, buffer, sem, s):
        slot = lax.rem(s, SLOTS)
        return pltpu.make_async_copy(hbm.at[s], buffer.at[slot], sem.at[slot])

    def in_pieces(hbm, buffer, sem, s):
        slot = lax.rem(s, SLOTS)
        size = buffer.shape[1] // 4
        for piece in range(4):
            rows = pl.ds(piece * size, size)
            pltpu.make_async_copy(hbm.at[s, rows], buffer.at[slot, rows], sem.at[slot]).start()

    def fetch_k(s):
        return fetch(k_hbm, keys, k_sem, s)

    def fetch_v(s):
        return fetch(v_hbm, values, v_sem, s)

    fetch_q = pltpu.make_async_copy(q_hbm, q_ref, q_sem)
    fetch_q.start()
    for u in range(STEP):
        fetch_k(u).start()
    for u in range(STEP):
        fetch_v(u).start()
    barrier = pltpu.get_barrier_semaphore()
    for d in order:
        pl.semaphore_signal(barrier, inc=1, device_id=device(lax.rem(me + d, devices)), device_id_type=pl.DeviceIdType.MESH)

    half = heads // 2
    own = lax.broadcasted_iota(jnp.int32, (half, 4 * depth), 0) // 4 == lax.broadcasted_iota(jnp.int32, (half, 4 * depth), 1) // depth
    lane = lax.broadcasted_iota(jnp.int32, (8, 128), 1)
    row = lax.broadcasted_iota(jnp.int32, (8, 128), 0)
    left, upper = lane < 64, row < 4
    lane32 = lax.broadcasted_iota(jnp.int32, (32, 128), 1)
    row32 = lax.broadcasted_iota(jnp.int32, (32, 128), 0)
    place = lax.rem(row32 // 4, 2) * 16 + row32 // 8 * 4 + lax.rem(row32, 4)
    lane16 = lax.broadcasted_iota(jnp.int32, (16, 128), 1)
    row16 = lax.broadcasted_iota(jnp.int32, (16, 128), 0)

    def score(s, slot):
        q = q_ref[s]
        q = jnp.concatenate([q, q], 1)
        q = jnp.concatenate([q, q], 1)
        for g in range(2):
            rows = pl.ds(half * g, half)
            mine = jnp.where(own, q[half * g : half * (g + 1)].astype(jnp.float32), 0.0).astype(jnp.bfloat16)
            block = keys[lax.rem(s, SLOTS), pl.ds(4 * depth * g, 4 * depth), :]
            scores[slot, rows, :] = jnp.dot(mine, block, preferred_element_type=jnp.float32)

    def attend(s, slot):
        seen, highs, totals = [], [], []
        for g in range(2):
            x = scores[slot, pl.ds(half * g, half), :]
            high = jnp.max(x, -1, keepdims=True)
            weights = jnp.exp2((x - high) * factor)
            highs.append(high)
            totals.append(jnp.sum(weights, -1, keepdims=True))
            block = values[lax.rem(s, SLOTS), pl.ds(4 * depth * g, 4 * depth), :]
            o = lax.dot_general(weights.astype(jnp.bfloat16), block, (((1,), (1,)), ((), ())), preferred_element_type=jnp.float32)
            a, b = o[:8, :128], o[8:, 128:]
            a = jnp.where(left, a, pltpu.roll(a, 4, 0))
            b = jnp.where(left, pltpu.roll(b, 4, 0), b)
            seen.append(jnp.where(upper, a, b))
        part[s] = jnp.concatenate(seen, 0).astype(jnp.bfloat16)
        both = jnp.where(lane32 == place, jnp.concatenate(highs, 0), 0.0) + jnp.where(lane32 == place + 32, jnp.concatenate(totals, 0), 0.0)
        stat[s] = jnp.sum(both, 0, keepdims=True)

    def first_of(d):
        return spread + (front - 1 - d) * STEP

    def remote(src, dst, send, recv, to):
        return pltpu.make_async_remote_copy(src, dst, send, recv, device(to), pl.DeviceIdType.MESH)

    neighbour = lax.rem(me + 1, devices)

    def leave(i):
        j = i - spread // STEP
        for u in range(STEP):
            s = i * STEP + u
            owner = jnp.where(j < 0, lax.rem(s, front), jnp.maximum(0, front - 1 - j))
            slot = jnp.where(j < 0, s // front, turns + u + jnp.maximum(0, j - front + 1) * STEP)

            mine = owner == me
            to, sem = jnp.where(mine, neighbour, owner), jnp.where(mine, most_own, slot)
            slot = jnp.where(mine, most_own + slot, slot)
            remote(part.at[s], owner_parts.at[me, slot], send_part.at[0], owner_recv_part.at[sem], to).start()
            remote(stat.at[s], owner_stats.at[me, slot], send_stat.at[0], owner_recv_stat.at[sem], to).start()

    def leave_all(s):
        here, there = pl.ds(s, STEP), pl.ds(s - shared, STEP)
        for d in order:
            to = lax.rem(me + d, devices)
            remote(part.at[here], parts.at[me, there], send_part.at[1], recv_part, to).start()
            remote(stat.at[here], stats.at[me, there], send_stat.at[1], recv_stat, to).start()


    def arrived(part_block, stat_block, part_sem, stat_sem):
        remote(part_block, part_block, send_part.at[0], part_sem, neighbour).wait_recv()
        remote(stat_block, stat_block, send_stat.at[0], stat_sem, neighbour).wait_recv()

    most = pl.ds(0, devices - 1)

    def together(parts, stats, slot, s):
        parts[me, slot] = part[s]
        stats[me, slot] = stat[s]
        st = stats[:, slot].reshape(devices, 128)
        scale = jnp.exp2((st - jnp.max(st, 0, keepdims=True)) * factor)
        total = jnp.sum(scale * pltpu.roll(st, 96, 1), 0, keepdims=True)
        scale = scale / total
        out = jnp.zeros((16, 128), jnp.float32)
        for j in range(devices):
            one = scale[j : j + 1]
            even = jnp.sum(jnp.where(lane16 == row16, one, 0.0), 1, keepdims=True)
            odd = jnp.sum(jnp.where(lane16 == row16 + 16, one, 0.0), 1, keepdims=True)
            out = out + parts[j, slot].astype(jnp.float32) * jnp.where(lane16 < 64, even, odd)
        return out

    def write(s, x):
        rows = []
        for j in range(2):
            v = x[8 * j : 8 * (j + 1)]
            w = pltpu.roll(v, 64, 1)
            rows += [jnp.where(upper, v, pltpu.roll(w, 4, 0)), jnp.where(upper, pltpu.roll(v, 4, 0), w)]
        out_ref[s] = jnp.concatenate(rows, 0).astype(jnp.bfloat16)

    def share(s, slot, group):
        arrived(owner_parts.at[most, 0], owner_stats.at[most, 0], owner_recv_part.at[slot], owner_recv_stat.at[slot])
        done[s] = together(owner_parts, owner_stats, slot, s).astype(jnp.bfloat16)
        for d in reversed(order):
            remote(done.at[s], done.at[s], send_done, recv_done.at[group], lax.rem(me + d, devices)).start()

    fetch_q.wait()
    for u in range(STEP):
        fetch_k(STEP + u).start()
    for u in range(STEP):
        fetch_k(u).wait()
        score(u, u)
        for t in range(STEP):
            (fetch_k(2 * STEP + t) if u else fetch_v(STEP + t)).start()
    for u in range(STEP):
        fetch_v(u).wait()
    for u in range(STEP):
        attend(u, u)
    for u in range(STEP):
        fetch_v(2 * STEP + u).start()
        fetch_k(3 * STEP + u).start()
    for u in range(STEP):
        fetch_k(STEP + u).wait()
    for u in range(STEP):
        score(STEP + u, STEP + u)
    for u in range(STEP):
        fetch_v(3 * STEP + u).start()
        fetch_k(4 * STEP + u).start()

    steps = sequences // STEP

    def body(i, leaves, refill):
        s = i * STEP
        now = lax.rem(i, 2) * STEP
        for u in range(STEP):
            fetch_k(s + STEP + u).wait()
            fetch_v(s + u).wait()
        if leaves:
            leave(i - 1)
        for u in range(STEP):
            score(s + STEP + u, STEP - now + u)
        for u in range(STEP):
            attend(s + u, now + u)
        if refill:
            for u in range(STEP):
                fetch_k(s + STEP + SLOTS + u).start()
                fetch_v(s + SLOTS + u).start()

    def early(i, _):
        body(i, False, True)
        return 0

    def later(i, _):
        body(i, True, True)
        return 0

    def first(i, _):
        leave(i)
        return 0

    full = (sequences - SLOTS) // STEP - 1
    lax.fori_loop(1, GREET, early, 0)
    pl.semaphore_wait(barrier, devices - 1)
    lax.fori_loop(0, GREET - 1, first, 0)
    lax.fori_loop(GREET, full, later, 0)
    for i in range(full, steps - 1):
        body(i, True, False)
        if i == full:
            in_pieces(v_hbm, values, v_sem, i * STEP + SLOTS)
            for u in range(1, STEP):
                fetch_v(i * STEP + SLOTS + u).start()
    leave(steps - 2)
    last = sequences - STEP
    for u in range(STEP):
        fetch_v(last + u).wait()
        attend(last + u, last % (2 * STEP) + u)
    leave_all(last)

    def await_done(group, count):
        block = done.at[pl.ds(0, count)]
        remote(block, block, send_done, recv_done.at[group], neighbour).wait_recv()

    def emit(first, end):
        for s in range(first, end):
            write(s, done[s].astype(jnp.float32))

    is_owner, is_first, is_middle = me < front, me == 0, (me > 0) & (me < front)

    @pl.when(is_owner)
    def _():
        def each(t, _):
            share(t * front + me, t, 0)
            return 0

        lax.fori_loop(0, turns, each, 0)
        for u in range(STEP):
            share(first_of(me) + u, turns + u, 1)

    def sent(own):
        some, few = part.at[pl.ds(0, shared)], stat.at[pl.ds(0, shared)]
        remote(some, some, send_part.at[0], recv_part, neighbour).wait_send()
        remote(few, few, send_stat.at[0], recv_stat, neighbour).wait_send()
        if own:
            block = owner_parts.at[most, pl.ds(0, own)]
            remote(block, block, send_done, recv_part, neighbour).wait_send()

    def unread(count):
        arrived(part.at[pl.ds(0, count)], stat.at[pl.ds(0, count)], owner_recv_part.at[most_own], owner_recv_stat.at[most_own])

    @pl.when(me == 1)
    def _():
        unread(most_own)

    @pl.when((me > 1) & (me <= front))
    def _():
        unread(turns + STEP)

    @pl.when(is_first)
    def _():
        for u in range(STEP, 2 * STEP):
            share(first_of(0) + u, turns + u, 1)
        await_done(0, spread - turns)
        await_done(1, (front - 1) * STEP)
        sent(most_own)

    @pl.when(is_middle)
    def _():
        await_done(0, spread - turns)
        sent(turns + STEP)
        await_done(1, front * STEP)

    @pl.when(jnp.logical_not(is_owner))
    def _():
        await_done(0, spread)
        sent(0)
        await_done(1, (front + 1) * STEP)

    emit(0, shared)
    some_parts, some_stats = parts.at[most, pl.ds(0, STEP)], stats.at[most, pl.ds(0, STEP)]
    remote(some_parts, some_parts, send_part.at[1], recv_part, neighbour).wait()
    remote(some_stats, some_stats, send_stat.at[1], recv_stat, neighbour).wait()
    for u in range(STEP):
        write(shared + u, together(parts, stats, u, shared + u))


def solution(mesh):
    devices = mesh.shape["sp"]

    def step(q, k, v):
        n, heads, depth = q.shape
        tokens, groups = k.shape[1:3]
        shared = n - DIRECT
        own = (shared - (devices // 2 + 1) * STEP) // (devices // 2) + 2 * STEP
        k, v = (x.transpose(0, 2, 3, 1).reshape(n, groups * depth, tokens) for x in (k, v))
        out = pl.pallas_call(
            functools.partial(kernel, devices),
            out_shape=pltpu.VMEM((n, heads, 128), jnp.bfloat16),
            in_specs=[pl.BlockSpec(memory_space=pl.ANY)] * 3,
            out_specs=pl.BlockSpec(memory_space=pltpu.VMEM),
            scratch_shapes=[
                pltpu.VMEM((n, heads, depth), jnp.bfloat16),
                pltpu.VMEM((SLOTS, groups * depth, tokens), jnp.bfloat16),
                pltpu.VMEM((SLOTS, groups * depth, tokens), jnp.bfloat16),
                pltpu.VMEM((2 * STEP, heads, tokens), jnp.float32),
                pltpu.VMEM((n, 16, 128), jnp.bfloat16),
                pltpu.VMEM((n, 1, 128), jnp.float32),
                pltpu.VMEM((devices, 2 * own, 16, 128), jnp.bfloat16),
                pltpu.VMEM((devices, 2 * own, 1, 128), jnp.float32),
                pltpu.VMEM((devices, DIRECT, 16, 128), jnp.bfloat16),
                pltpu.VMEM((devices, DIRECT, 1, 128), jnp.float32),
                pltpu.VMEM((shared, 16, 128), jnp.bfloat16),
                pltpu.SemaphoreType.DMA,
                pltpu.SemaphoreType.DMA((SLOTS,)),
                pltpu.SemaphoreType.DMA((SLOTS,)),
                pltpu.SemaphoreType.DMA((2,)),
                pltpu.SemaphoreType.DMA((2,)),
                pltpu.SemaphoreType.DMA((own + 1,)),
                pltpu.SemaphoreType.DMA((own + 1,)),
                pltpu.SemaphoreType.DMA,
                pltpu.SemaphoreType.DMA,
                pltpu.SemaphoreType.DMA,
                pltpu.SemaphoreType.DMA((2,)),
            ],
            compiler_params=pltpu.CompilerParams(collective_id=0, has_side_effects=True, vmem_limit_bytes=60 * 2**20),
        )(q, k, v)
        return out[:, :, :depth]

    return jax.shard_map(
        step,
        mesh=mesh,
        in_specs=(P("dp", None, None), P("dp", "sp", None, None), P("dp", "sp", None, None)),
        out_specs=P("dp", None, None),
        check_vma=False,
    )
```
